32 devices in a mesh: dp: 1 (over z), fsdp: 32 (over y, x, core).
Axes of the slice: x: 4, y: 4, z: 1, core: 2. Of those that a mesh axis runs over, the one named last changes fastest.
The devices are a block of a 4x4x8 slice.
Arguments:
- x: bfloat16 [32, 64, 2048], P(('dp', 'fsdp'))
- gain: bfloat16 [2, 2048], replicated
- w_in: bfloat16 [2, 2048, 18944], P(None, None, 'fsdp')
- w_out: bfloat16 [2, 10240, 2048], P(None, 'fsdp')
Outputs:
- output 1: bfloat16 [32, 64, 2048], P(('dp', 'fsdp'))
- output 2: bfloat16 [2, 32, 64, 256], P(None, ('dp', 'fsdp'))
- output 3: bfloat16 [2, 32, 64, 256], P(None, ('dp', 'fsdp'))
All inputs are finite; a program needn't handle non-finite values.
Results may differ from the reference program's by a relative error of at most 0.0128833.
Values are sent between devices in bfloat16 or wider.
A program may use at most 768 MiB of HBM per device.

```python
import jax
import jax.numpy as jnp
from jax import lax

BATCH_SEQS = 32
SEQ_LEN = 64
D_MODEL = 2048
NUM_HEADS = 8
FF_DIM = 8192
HEAD_DIM = 256
NUM_LAYERS = 2
Q_COLS = NUM_HEADS * HEAD_DIM
IN_COLS = Q_COLS + 2 * HEAD_DIM + 2 * FF_DIM
OUT_ROWS = Q_COLS + FF_DIM
ROPE_BASE = 10000.0
NORM_EPS = 1e-6


def normal_weight(key, rows, cols):
    return (jax.random.normal(key, (rows, cols), jnp.float32) * rows ** -0.5).astype(jnp.bfloat16)


def setup_inputs(seed: int = 0, part: int = 0) -> dict:
    key = jax.random.key(seed)
    act_key = jax.random.fold_in(jax.random.fold_in(key, 1), part)
    gain_key, in_key, out_key = jax.random.split(jax.random.fold_in(key, 2), 3)
    in_keys = jax.random.split(in_key, NUM_LAYERS)
    out_keys = jax.random.split(out_key, NUM_LAYERS)
    x = (0.5 * jax.random.normal(act_key, (BATCH_SEQS, SEQ_LEN, D_MODEL), jnp.float32)).astype(jnp.bfloat16)
    gain = (1.0 + 0.3 * jax.random.normal(gain_key, (NUM_LAYERS, D_MODEL), jnp.float32)).astype(jnp.bfloat16)
    w_in = jnp.stack([normal_weight(in_keys[layer], D_MODEL, IN_COLS) for layer in range(NUM_LAYERS)])
    w_out = jnp.stack([normal_weight(out_keys[layer], OUT_ROWS, D_MODEL) for layer in range(NUM_LAYERS)])
    return {"x": x, "gain": gain, "w_in": w_in, "w_out": w_out}


def rope_tables():
    half_dim = HEAD_DIM // 2
    inv_freq = ROPE_BASE ** (-jnp.arange(half_dim, dtype=jnp.float32) / half_dim)
    angle = jnp.arange(SEQ_LEN, dtype=jnp.float32)[:, None] * inv_freq[None, :]
    return jnp.cos(angle), jnp.sin(angle)


def apply_rope(tensor, cos_table, sin_table):
    half_dim = HEAD_DIM // 2
    first = tensor[..., :half_dim]
    second = tensor[..., half_dim:]
    return jnp.concatenate([first * cos_table - second * sin_table, second * cos_table + first * sin_table], axis=-1)


def layer_norm(hidden, gain_vec):
    x_float = hidden.astype(jnp.float32)
    centred = x_float - jnp.mean(x_float, axis=-1, keepdims=True)
    variance = jnp.mean(centred * centred, axis=-1, keepdims=True)
    return (centred * lax.rsqrt(variance + NORM_EPS) * gain_vec.astype(jnp.float32)).astype(jnp.bfloat16)


def layer_step(hidden, layer_weights):
    gain_vec, w_in_layer, w_out_layer = layer_weights
    normed = layer_norm(hidden, gain_vec)
    projected = jnp.dot(normed, w_in_layer, preferred_element_type=jnp.float32).astype(jnp.bfloat16)
    query = projected[:, :Q_COLS].reshape(SEQ_LEN, NUM_HEADS, HEAD_DIM)
    key_raw = projected[:, Q_COLS:Q_COLS + HEAD_DIM]
    value = projected[:, Q_COLS + HEAD_DIM:Q_COLS + 2 * HEAD_DIM]
    gate = projected[:, Q_COLS + 2 * HEAD_DIM:Q_COLS + 2 * HEAD_DIM + FF_DIM]
    up_proj = projected[:, Q_COLS + 2 * HEAD_DIM + FF_DIM:]
    cos_table, sin_table = rope_tables()
    q_rot = (apply_rope(query.astype(jnp.float32), cos_table[:, None, :], sin_table[:, None, :]) * HEAD_DIM ** -0.5).astype(jnp.bfloat16)
    k_rot = apply_rope(key_raw.astype(jnp.float32), cos_table, sin_table).astype(jnp.bfloat16)
    scores = jnp.einsum("qhd,kd->qhk", q_rot.astype(jnp.float32), k_rot.astype(jnp.float32))
    causal = jnp.arange(SEQ_LEN)[:, None, None] >= jnp.arange(SEQ_LEN)[None, None, :]
    scores = jnp.where(causal, scores, -1e30)
    exp_scores = jnp.exp(scores - jnp.max(scores, axis=-1, keepdims=True))
    row_sum = jnp.sum(exp_scores, axis=-1, keepdims=True)
    attended = jnp.einsum("qhk,kd->qhd", exp_scores.astype(jnp.bfloat16).astype(jnp.float32), value.astype(jnp.float32)) / row_sum
    attended = attended.astype(jnp.bfloat16).reshape(SEQ_LEN, Q_COLS)
    gated = (jax.nn.silu(gate.astype(jnp.float32)) * up_proj.astype(jnp.float32)).astype(jnp.bfloat16)
    mixed = jnp.concatenate([attended, gated], axis=-1)
    out_sum = jnp.dot(mixed, w_out_layer, preferred_element_type=jnp.float32)
    new_hidden = (hidden.astype(jnp.float32) + out_sum).astype(jnp.bfloat16)
    return new_hidden, (k_rot, value)


def reference(x, gain, w_in, w_out):
    def run_sequence(seq_x):
        final, caches = lax.scan(layer_step, seq_x, (gain, w_in, w_out))
        return final, caches[0], caches[1]
    hidden, key_cache, value_cache = lax.map(run_sequence, x)
    return hidden, jnp.transpose(key_cache, (1, 0, 2, 3)), jnp.transpose(value_cache, (1, 0, 2, 3))
```

```python
import jax
import jax.numpy as jnp
from jax import lax
from jax.sharding import PartitionSpec as P

HEAD_DIM = 256
ROPE_BASE = 10000.0
NORM_EPS = 1e-6


def layer_norm(hidden, gain_vec):
    x_float = hidden.astype(jnp.float32)
    centred = x_float - jnp.mean(x_float, axis=-1, keepdims=True)
    variance = jnp.mean(centred * centred, axis=-1, keepdims=True)
    return (centred * lax.rsqrt(variance + NORM_EPS) * gain_vec.astype(jnp.float32)).astype(jnp.bfloat16)


def rope_tables(seq_len):
    half_dim = HEAD_DIM // 2
    inv_freq = ROPE_BASE ** (-jnp.arange(half_dim, dtype=jnp.float32) / half_dim)
    angle = jnp.arange(seq_len, dtype=jnp.float32)[:, None] * inv_freq[None, :]
    return jnp.cos(angle), jnp.sin(angle)


def apply_rope(tensor, cos_table, sin_table):
    half_dim = HEAD_DIM // 2
    first = tensor[..., :half_dim]
    second = tensor[..., half_dim:]
    return jnp.concatenate([first * cos_table - second * sin_table, second * cos_table + first * sin_table], axis=-1)


def mix_tokens(projected, num_heads, ff_dim):
    batch, seq_len, _ = projected.shape
    q_cols = num_heads * HEAD_DIM
    query = projected[..., :q_cols].reshape(batch, seq_len, num_heads, HEAD_DIM)
    key_raw = projected[..., q_cols:q_cols + HEAD_DIM]
    value = projected[..., q_cols + HEAD_DIM:q_cols + 2 * HEAD_DIM]
    gate = projected[..., q_cols + 2 * HEAD_DIM:q_cols + 2 * HEAD_DIM + ff_dim]
    up_proj = projected[..., q_cols + 2 * HEAD_DIM + ff_dim:]
    cos_table, sin_table = rope_tables(seq_len)
    q_rot = (apply_rope(query.astype(jnp.float32), cos_table[:, None, :], sin_table[:, None, :]) * HEAD_DIM ** -0.5).astype(jnp.bfloat16)
    k_rot = apply_rope(key_raw.astype(jnp.float32), cos_table, sin_table).astype(jnp.bfloat16)
    scores = jnp.einsum("crie,cle->cril", q_rot, k_rot, preferred_element_type=jnp.float32)
    causal = jnp.arange(seq_len)[:, None, None] >= jnp.arange(seq_len)[None, None, :]
    scores = jnp.where(causal, scores, -1e30)
    exp_scores = jnp.exp(scores - jnp.max(scores, axis=-1, keepdims=True))
    row_sum = jnp.sum(exp_scores, axis=-1, keepdims=True)
    attended = jnp.einsum("cril,cle->crie", exp_scores.astype(jnp.bfloat16), value, preferred_element_type=jnp.float32) / row_sum
    attended = attended.astype(jnp.bfloat16).reshape(batch, seq_len, q_cols)
    gated = (jax.nn.silu(gate.astype(jnp.float32)) * up_proj.astype(jnp.float32)).astype(jnp.bfloat16)
    return attended, gated, k_rot, value


def parallel_layer(hidden, gain_vec, w_in_part, w_out_part, group):
    batch, seq_len, d_model = hidden.shape
    in_part = w_in_part.shape[1]
    out_part = w_out_part.shape[0]
    out_rows = out_part * group
    ff_dim = in_part * group - out_rows - 2 * HEAD_DIM
    num_heads = (out_rows - ff_dim) // HEAD_DIM
    tokens = batch * seq_len
    normed = layer_norm(hidden, gain_vec).reshape(tokens, d_model)
    normed_all = lax.all_gather(normed, "fsdp", axis=0, tiled=True)
    projected = jnp.dot(normed_all, w_in_part, preferred_element_type=jnp.float32).astype(jnp.bfloat16)
    projected = lax.all_to_all(projected.reshape(group, tokens, in_part), "fsdp", 0, 0, tiled=True)
    projected = jnp.transpose(projected, (1, 0, 2)).reshape(batch, seq_len, group * in_part)
    attended, gated, k_rot, value = mix_tokens(projected, num_heads, ff_dim)
    mixed = jnp.concatenate([attended, gated], axis=-1).reshape(tokens, group, out_part)
    mixed = lax.all_to_all(jnp.transpose(mixed, (1, 0, 2)), "fsdp", 0, 0, tiled=True)
    partial = jnp.dot(mixed.reshape(group * tokens, out_part), w_out_part, preferred_element_type=jnp.float32)
    out_sum = lax.psum_scatter(partial, "fsdp", scatter_dimension=0, tiled=True)
    new_hidden = (hidden.astype(jnp.float32) + out_sum.reshape(hidden.shape)).astype(jnp.bfloat16)
    return new_hidden, k_rot, value


def solution(mesh):
    batch_axes = ("dp", "fsdp")

    def device_program(x_local, gain, w_in_local, w_out_local):
        hidden = x_local
        key_list = []
        value_list = []
        for layer in range(w_in_local.shape[0]):
            hidden, k_rot, value = parallel_layer(hidden, gain[layer], w_in_local[layer], w_out_local[layer], mesh.shape["fsdp"])
            key_list.append(k_rot)
            value_list.append(value)
        return hidden, jnp.stack(key_list), jnp.stack(value_list)

    return jax.shard_map(
        device_program,
        mesh=mesh,
        in_specs=(P(batch_axes, None, None), P(None, None), P(None, None, "fsdp"), P(None, "fsdp", None)),
        out_specs=(P(batch_axes, None, None), P(None, batch_axes, None, None), P(None, batch_axes, None, None)),
        check_vma=False,
    )
```

```python
import functools
import math

import jax
import jax.numpy as jnp
from jax import lax
from jax.experimental import pallas as pl
from jax.experimental.pallas import tpu as pltpu
from jax.sharding import PartitionSpec as P

HEAD_DIM = 256
ROPE_BASE = 10000.0
NORM_EPS = 1e-6
LANES = 128
CORES = 2
MESH = pl.DeviceIdType.MESH


def rope_tables(seq_len):
    half_dim = HEAD_DIM // 2
    inv_freq = ROPE_BASE ** (-jnp.arange(half_dim, dtype=jnp.float32) / half_dim)
    angle = jnp.arange(seq_len, dtype=jnp.float32)[:, None] * inv_freq[None, :]
    return jnp.cos(angle), jnp.sin(angle)


GATHER, SEND_P, SEND_M, REDUCE, WEIGHT = 0, 40, 56, 72, 96
EVENTS = 98


def layer_kernel(ring, num_heads, x_ref, gain_ref, w_in_ref, w_out_ref, cos_ref, sin_ref, y_ref, k_ref, v_ref,
                 h_all, w_in_own, w_in_peer, w_out_all, p_out, p_in, mixed_out, mixed_in, part_y, part_x,
                 opp_lo, opp_hi, ring_lo, ring_hi, last_opp_lo, last_opp_hi, last_lo, last_hi,
                 send_sem, recv_sem, local_sem):
    tokens, d_model = x_ref.shape
    half, quarter = tokens // 2, tokens // 4
    d_half = d_model // 2
    out_part = w_out_ref.shape[0]
    chip_rows = CORES * out_part
    chip_cols = w_in_ref.shape[1]
    me = lax.axis_index("fsdp")
    core = lax.rem(me, CORES)
    chip = me // CORES
    x = lax.rem(chip, ring)
    y = chip // ring

    def wrap(a):
        return lax.rem(a + ring, ring)

    def device(cx, cy):
        return (wrap(cy) * ring + wrap(cx)) * CORES + core

    sends = []
    done = set()

    def send(event, src, dst, target):
        copy = pltpu.make_async_remote_copy(src_ref=src, dst_ref=dst, send_sem=send_sem.at[event],
                                            recv_sem=recv_sem.at[event], device_id={"fsdp": target},
                                            device_id_type=MESH)
        copy.start()
        sends.append(copy)

    def need(event, dst):
        if event in done:
            return
        done.add(event)
        pltpu.make_async_remote_copy(src_ref=dst, dst_ref=dst, send_sem=send_sem.at[event],
                                     recv_sem=recv_sem.at[event], device_id={"fsdp": me},
                                     device_id_type=MESH).wait_recv()

    peer = chip * CORES + (1 - core)
    barrier = pltpu.get_barrier_semaphore()
    pl.semaphore_signal(barrier, inc=1, device_id={"fsdp": peer}, device_id_type=MESH)
    others = [(dx, dy) for dy in range(ring) for dx in range(ring) if dx or dy]
    for dx, dy in others:
        pl.semaphore_signal(barrier, inc=1, device_id={"fsdp": device(x + dx, y + dy)}, device_id_type=MESH)

    local = [
        pltpu.make_async_copy(w_in_ref, w_in_own, local_sem.at[0]),
        pltpu.make_async_copy(w_out_ref, w_out_all.at[pl.ds(core * out_part, out_part)], local_sem.at[1]),
    ]
    for copy in local:
        copy.start()

    x_float = x_ref[...].astype(jnp.float32)
    centred = x_float - jnp.mean(x_float, axis=-1, keepdims=True)
    variance = jnp.mean(centred * centred, axis=-1, keepdims=True)
    normed = centred * lax.rsqrt(variance + NORM_EPS) * gain_ref[...].astype(jnp.float32)
    h_all[y, x] = normed.astype(jnp.bfloat16)

    pl.semaphore_wait(barrier, len(others) + 1)

    def place(part, prim, sec):
        return (x + prim, y + sec) if part == 0 else (x + sec, y + prim)

    def block(part, prim, sec, low, count):
        cx, cy = place(part, prim, sec)
        return h_all.at[wrap(cy), wrap(cx), pl.ds(part * half + low, count)]

    def gather_send(event, part, blk, prim, sec):
        send(event, blk, blk, device(*place(part, prim, sec)))

    steps = (0, -1, 1, 2)

    def base(part):
        return GATHER + 20 * part

    def to_second(part, j):
        e = base(part) + 4 + 4 * j
        blk = block(part, steps[j], 0, 0, half)
        gather_send(e, part, blk, 0, 1)
        gather_send(e + 1, part, blk, 0, -1)

    def got_first(part, which):
        e = base(part)
        if which == -1:
            need(e, block(part, -1, 0, 0, half))
        elif which == 1:
            need(e + 1, block(part, 1, 0, 0, half))
        else:
            need(e + 2, block(part, 2, 0, 0, quarter))
            need(e + 3, block(part, 2, 0, quarter, quarter))

    def got_second(part, j, which):
        e = base(part) + 4 + 4 * j
        dp = steps[j]
        if which == -1:
            need(e, block(part, dp, -1, 0, half))
        elif which == 1:
            need(e + 1, block(part, dp, 1, 0, half))
        else:
            need(e + 2, block(part, dp, 2, 0, quarter))
            need(e + 3, block(part, dp, 2, quarter, quarter))

    def pass_second(part, j):
        e = base(part) + 4 + 4 * j
        dp = steps[j]
        got_second(part, j, -1)
        gather_send(e + 2, part, block(part, dp, -1, 0, quarter), 0, 1)
        got_second(part, j, 1)
        gather_send(e + 3, part, block(part, dp, 1, quarter, quarter), 0, -1)

    for part in (0, 1):
        own = block(part, 0, 0, 0, half)
        gather_send(base(part), part, own, 1, 0)
        gather_send(base(part) + 1, part, own, -1, 0)
    for part in (0, 1):
        to_second(part, 0)
    send(WEIGHT, w_in_ref, w_in_peer, peer)
    send(WEIGHT + 1, w_out_ref, w_out_all.at[pl.ds(core * out_part, out_part)], peer)
    for part in (0, 1):
        got_first(part, -1)
        gather_send(base(part) + 2, part, block(part, -1, 0, 0, quarter), 1, 0)
        got_first(part, 1)
        gather_send(base(part) + 3, part, block(part, 1, 0, quarter, quarter), -1, 0)
    for part in (0, 1):
        to_second(part, 1)
        to_second(part, 2)
    for part in (0, 1):
        pass_second(part, 0)
    for part in (0, 1):
        got_first(part, 2)
        to_second(part, 3)

    local[0].wait()
    need(WEIGHT, w_in_peer)
    strip = min(d_model, 256)

    @pl.loop(0, d_model // strip)
    def _(i):
        rows = pl.ds(pl.multiple_of(i * strip, strip), strip)
        w_in_own[rows] = w_in_own[rows] + w_in_peer[rows]

    wide = math.gcd(chip_cols, 256)

    def row_product(dy):
        row = wrap(y + dy)
        lhs = h_all[row].reshape(ring * tokens, d_model)

        @pl.loop(0, chip_cols // wide)
        def _(n):
            cols = pl.ds(pl.multiple_of(n * wide, wide), wide)
            res = jnp.dot(lhs, w_in_own[:, cols], preferred_element_type=jnp.float32)
            p_out[row, :, :, cols] = res.astype(jnp.bfloat16).reshape(ring, tokens, wide)

        for dx in (2, 1, 3, 0):
            col = wrap(x + dx)
            if dx == 0 and dy == 0:
                p_in[y, x] = p_out[y, x]
            else:
                send(SEND_P + (dy % ring) * ring + dx, p_out.at[row, col], p_in.at[y, x], device(x + dx, y + dy))

    for which in (-1, 1, 2):
        got_second(1, 0, which)
    row_product(0)
    for j in (1, 2):
        for part in (0, 1):
            pass_second(part, j)
    for part in (0, 1):
        pass_second(part, 3)
    for dy, j in ((-1, 1), (1, 2), (2, 3)):
        for i in range(ring):
            got_second(0, i, dy)
        for which in (-1, 1, 2):
            got_second(1, j, which)
        row_product(dy)

    for dx, dy in others:
        need(SEND_P + dy * ring + dx, p_in.at[wrap(y - dy), wrap(x - dx)])

    real_cols = chip_cols_real(w_in_ref, ring, num_heads, out_part)

    def tile(t):
        pieces = []
        for c in range(ring * ring):
            if c * real_cols < (t + 1) * LANES and (c + 1) * real_cols > t * LANES:
                low = (t - (c * real_cols) // LANES) * LANES
                pieces.append(p_in[c // ring, c % ring, :, low:low + LANES])
        return sum(pieces[1:], pieces[0])

    cos_table = cos_ref[...]
    sin_table = sin_ref[...]

    def rotated(t, scale):
        first = tile(t).astype(jnp.float32)
        second = tile(t + 1).astype(jnp.float32)
        a = first * cos_table - second * sin_table
        b = second * cos_table + first * sin_table
        return jnp.concatenate([(a * scale).astype(jnp.bfloat16), (b * scale).astype(jnp.bfloat16)], axis=-1)

    head_tiles = HEAD_DIM // LANES
    q_tiles = num_heads * head_tiles
    out_tiles = chip_rows // LANES

    def put(t, val):
        c, i = divmod(t, out_tiles)
        mixed_out[c, :, i * LANES:(i + 1) * LANES] = val

    query = jnp.concatenate([rotated(h * head_tiles, HEAD_DIM ** -0.5) for h in range(num_heads)], axis=0)
    key = rotated(q_tiles, 1.0)
    value = jnp.concatenate([tile(q_tiles + 2), tile(q_tiles + 3)], axis=-1)
    k_ref[...] = key
    v_ref[...] = value
    scores = lax.dot_general(query, key, (((1,), (1,)), ((), ())), preferred_element_type=jnp.float32)
    scores = scores.reshape(num_heads, tokens, tokens)
    q_pos = lax.broadcasted_iota(jnp.int32, scores.shape, 1)
    k_pos = lax.broadcasted_iota(jnp.int32, scores.shape, 2)
    scores = jnp.where(q_pos >= k_pos, scores, -1e30)
    weight = jnp.exp(scores - jnp.max(scores, axis=-1, keepdims=True))
    row_sum = jnp.sum(weight, axis=-1, keepdims=True)
    attended = jnp.dot(weight.astype(jnp.bfloat16).reshape(num_heads * tokens, tokens), value,
                       preferred_element_type=jnp.float32).reshape(num_heads, tokens, HEAD_DIM)
    attended = (attended / row_sum).astype(jnp.bfloat16)
    for h in range(num_heads):
        for i in range(head_tiles):
            put(h * head_tiles + i, attended[h, :, i * LANES:(i + 1) * LANES])
    ff_tiles = ring * ring * out_tiles - q_tiles
    for t in range(ff_tiles):
        gate = tile(q_tiles + 4 + t).astype(jnp.float32)
        up = tile(q_tiles + 4 + ff_tiles + t).astype(jnp.float32)
        put(q_tiles + t, (jax.nn.silu(gate) * up).astype(jnp.bfloat16))

    far_first = sorted(others, key=lambda d: -((d[0] == 2) + (d[1] == 2)))
    for dx, dy in far_first:
        send(SEND_M + dy * ring + dx, mixed_out.at[wrap(y + dy) * ring + wrap(x + dx)], mixed_in.at[y, x],
             device(x + dx, y + dy))
    mixed_in[y, x] = mixed_out[chip]
    local[1].wait()
    need(WEIGHT + 1, w_out_all.at[pl.ds((1 - core) * out_part, out_part)])

    parts = (part_y, part_x)
    centre = ((y, x), (x, y))

    def lined(f, prim, sec):
        return (x + sec, y + prim) if f == 0 else (x + prim, y + sec)

    def arrived(f, prim):
        for sec in range(ring):
            dx, dy = (-sec, -prim) if f == 0 else (-prim, -sec)
            dx, dy = dx % ring, dy % ring
            if dx or dy:
                need(SEND_M + dy * ring + dx, mixed_in.at[wrap(y - dy), wrap(x - dx)])

    narrow = min(d_half, 256)

    def product(f, prim):
        arrived(f, prim)
        idx = wrap(centre[f][0] + prim)
        lhs = mixed_in[idx] if f == 0 else mixed_in[:, idx]
        lhs = lhs.reshape(ring * tokens, chip_rows)

        @pl.loop(0, d_half // narrow)
        def _(n):
            src = pl.ds(pl.multiple_of(f * d_half + n * narrow, narrow), narrow)
            cols = pl.ds(pl.multiple_of(n * narrow, narrow), narrow)
            res = jnp.dot(lhs, w_out_all[:, src], preferred_element_type=jnp.float32)
            parts[f][idx, :, :, cols] = res.reshape(ring, tokens, narrow)

    lo, hi = pl.ds(0, ring // 2), pl.ds(ring // 2, ring // 2)
    t_lo, t_hi = pl.ds(0, half), pl.ds(half, half)

    def event(f, i):
        return REDUCE + 12 * f + i

    def at(f, prim):
        return wrap(centre[f][0] + prim)

    def toward(f, prim, sec):
        return device(*lined(f, prim, sec))

    for f in (0, 1):
        product(f, 2)
        send(event(f, 0), parts[f].at[at(f, 2), lo], opp_lo.at[f], toward(f, 1, 0))
        send(event(f, 1), parts[f].at[at(f, 2), hi], opp_hi.at[f], toward(f, -1, 0))
    for f in (0, 1):
        product(f, 1)
        send(event(f, 2), parts[f].at[at(f, 1), hi], ring_lo.at[f, hi], toward(f, 1, 0))
        product(f, -1)
        send(event(f, 3), parts[f].at[at(f, -1), lo], ring_hi.at[f, lo], toward(f, -1, 0))
    for f in (0, 1):
        product(f, 0)
    for f in (0, 1):
        need(event(f, 0), opp_lo.at[f])
        parts[f][at(f, 1), lo] = parts[f][at(f, 1), lo] + opp_lo[f]
        send(event(f, 4), parts[f].at[at(f, 1), lo], ring_lo.at[f, lo], toward(f, 1, 0))
        need(event(f, 1), opp_hi.at[f])
        parts[f][at(f, -1), hi] = parts[f][at(f, -1), hi] + opp_hi[f]
        send(event(f, 5), parts[f].at[at(f, -1), hi], ring_hi.at[f, hi], toward(f, -1, 0))

    def second(f, sec):
        return wrap(centre[f][1] + sec)

    for f in (0, 1):
        need(event(f, 2), ring_lo.at[f, hi])
        need(event(f, 3), ring_hi.at[f, lo])
        need(event(f, 4), ring_lo.at[f, lo])
        need(event(f, 5), ring_hi.at[f, hi])
        mid = at(f, 0)
        parts[f][mid] = parts[f][mid] + ring_lo[f] + ring_hi[f]
        send(event(f, 6), parts[f].at[mid, second(f, 2), t_lo], last_opp_lo.at[f], toward(f, 0, 1))
        send(event(f, 7), parts[f].at[mid, second(f, 2), t_hi], last_opp_hi.at[f], toward(f, 0, -1))
        send(event(f, 8), parts[f].at[mid, second(f, 1), t_hi], last_lo.at[f, t_hi], toward(f, 0, 1))
        send(event(f, 9), parts[f].at[mid, second(f, -1), t_lo], last_hi.at[f, t_lo], toward(f, 0, -1))
    for f in (0, 1):
        mid = at(f, 0)
        need(event(f, 6), last_opp_lo.at[f])
        parts[f][mid, second(f, 1), t_lo] = parts[f][mid, second(f, 1), t_lo] + last_opp_lo[f]
        send(event(f, 10), parts[f].at[mid, second(f, 1), t_lo], last_lo.at[f, t_lo], toward(f, 0, 1))
        need(event(f, 7), last_opp_hi.at[f])
        parts[f][mid, second(f, -1), t_hi] = parts[f][mid, second(f, -1), t_hi] + last_opp_hi[f]
        send(event(f, 11), parts[f].at[mid, second(f, -1), t_hi], last_hi.at[f, t_hi], toward(f, 0, -1))
    for f in (0, 1):
        need(event(f, 8), last_lo.at[f, t_hi])
        need(event(f, 9), last_hi.at[f, t_lo])
        need(event(f, 10), last_lo.at[f, t_lo])
        need(event(f, 11), last_hi.at[f, t_hi])
        out_sum = parts[f][at(f, 0), second(f, 0)] + last_lo[f] + last_hi[f]
        cols = slice(f * d_half, (f + 1) * d_half)
        y_ref[:, cols] = (x_ref[:, cols].astype(jnp.float32) + out_sum).astype(jnp.bfloat16)
    for copy in sends:
        copy.wait_send()


def chip_cols_real(w_in_ref, ring, num_heads, out_part):
    ff_dim = ring * ring * CORES * out_part - num_heads * HEAD_DIM
    return (num_heads * HEAD_DIM + 2 * HEAD_DIM + 2 * ff_dim) // (ring * ring)


def parallel_layer(hidden, gain_vec, w_in_place, w_out_part, tables, ring, num_heads):
    batch, tokens, d_model = hidden.shape
    padded_cols = w_in_place.shape[1]
    out_part = w_out_part.shape[0]
    chip_rows = CORES * out_part
    d_half = d_model // 2
    bf16, f32 = jnp.bfloat16, jnp.float32
    vmem = pl.BlockSpec(memory_space=pltpu.VMEM)
    anywhere = pl.BlockSpec(memory_space=pl.ANY)
    out, k_rot, value = pl.pallas_call(
        functools.partial(layer_kernel, ring, num_heads),
        out_shape=(
            jax.ShapeDtypeStruct((tokens, d_model), bf16),
            jax.ShapeDtypeStruct((tokens, HEAD_DIM), bf16),
            jax.ShapeDtypeStruct((tokens, HEAD_DIM), bf16),
        ),
        in_specs=[vmem, vmem, anywhere, anywhere, vmem, vmem],
        out_specs=(vmem, vmem, vmem),
        scratch_shapes=[
            pltpu.VMEM((ring, ring, tokens, d_model), bf16),
            pltpu.VMEM((d_model, padded_cols), bf16),
            pltpu.VMEM((d_model, padded_cols), bf16),
            pltpu.VMEM((chip_rows, d_model), bf16),
            pltpu.VMEM((ring, ring, tokens, padded_cols), bf16),
            pltpu.VMEM((ring, ring, tokens, padded_cols), bf16),
            pltpu.VMEM((ring * ring, tokens, chip_rows), bf16),
            pltpu.VMEM((ring, ring, tokens, chip_rows), bf16),
            pltpu.VMEM((ring, ring, tokens, d_half), f32),
            pltpu.VMEM((ring, ring, tokens, d_half), f32),
            pltpu.VMEM((2, ring // 2, tokens, d_half), f32),
            pltpu.VMEM((2, ring // 2, tokens, d_half), f32),
            pltpu.VMEM((2, ring, tokens, d_half), f32),
            pltpu.VMEM((2, ring, tokens, d_half), f32),
            pltpu.VMEM((2, tokens // 2, d_half), f32),
            pltpu.VMEM((2, tokens // 2, d_half), f32),
            pltpu.VMEM((2, tokens, d_half), f32),
            pltpu.VMEM((2, tokens, d_half), f32),
            pltpu.SemaphoreType.DMA((EVENTS,)),
            pltpu.SemaphoreType.DMA((EVENTS,)),
            pltpu.SemaphoreType.DMA((2,)),
        ],
        compiler_params=pltpu.CompilerParams(collective_id=0, has_side_effects=True, vmem_limit_bytes=62 * 2 ** 20),
        name="layer",
    )(hidden.reshape(tokens, d_model), gain_vec.reshape(1, d_model), w_in_place, w_out_part, *tables)
    return out.reshape(hidden.shape), k_rot.reshape(batch, tokens, HEAD_DIM), value.reshape(batch, tokens, HEAD_DIM)


def solution(mesh):
    batch_axes = ("dp", "fsdp")
    group = mesh.shape["fsdp"]
    ring = math.isqrt(group // CORES)
    if ring != 4 or ring * ring * CORES != group:
        raise ValueError("unsupported group")

    def device_program(x_local, gain, w_in_local, w_out_local):
        layers, d_model, in_part = w_in_local.shape
        out_rows = w_out_local.shape[1] * group
        ff_dim = in_part * group - out_rows - 2 * HEAD_DIM
        num_heads = (out_rows - ff_dim) // HEAD_DIM
        chip_cols = CORES * in_part
        phases = max((chip_cols * c) % LANES for c in range(ring * ring))
        padded = -(-(chip_cols + phases) // LANES) * LANES
        me = lax.axis_index("fsdp")
        offset = lax.rem(chip_cols * (me // CORES), LANES) + in_part * lax.rem(me, CORES)
        hidden = x_local
        tables = rope_tables(x_local.shape[1])
        key_list = []
        value_list = []
        for layer in range(layers):
            w_in_place = lax.dynamic_update_slice(jnp.zeros((d_model, padded), w_in_local.dtype), w_in_local[layer],
                                                  (0, offset))
            hidden, k_rot, value = parallel_layer(hidden, gain[layer], w_in_place, w_out_local[layer], tables, ring,
                                                  num_heads)
            key_list.append(k_rot)
            value_list.append(value)
        return hidden, jnp.stack(key_list), jnp.stack(value_list)

    return jax.shard_map(
        device_program,
        mesh=mesh,
        in_specs=(P(batch_axes, None, None), P(None, None), P(None, None, "fsdp"), P(None, "fsdp", None)),
        out_specs=(P(batch_axes, None, None), P(None, batch_axes, None, None), P(None, batch_axes, None, None)),
        check_vma=False,
    )
```

```python
import functools
import math

import jax
import jax.numpy as jnp
from jax import lax
from jax.experimental import pallas as pl
from jax.experimental.pallas import tpu as pltpu
import numpy as np
from jax.sharding import PartitionSpec as P

HEAD_DIM = 256
ROPE_BASE = 10000.0
NORM_EPS = 1e-6
LANES = 128
CORES = 2
MESH = pl.DeviceIdType.MESH


def rope_tables(seq_len):
    half_dim = HEAD_DIM // 2
    inv_freq = np.float32(ROPE_BASE) ** (-np.arange(half_dim, dtype=np.float32) / np.float32(half_dim))
    angle = np.arange(seq_len, dtype=np.float32)[:, None] * inv_freq[None, :].astype(np.float32)
    return jnp.asarray(np.cos(angle), jnp.float32), jnp.asarray(np.sin(angle), jnp.float32)


GATHER, SEND_P, SEND_M, REDUCE, WEIGHT = 0, 40, 56, 72, 96
EVENTS = 98


def layer_kernel(ring, num_heads, layer, x_ref, gain_ref, w_in_ref, w_out_ref, cos_ref, sin_ref, y_ref, k_ref, v_ref,
                 h_all, w_in_all, w_out_all, p_out, p_in, mixed_out, mixed_in, part_y, part_x,
                 opp_lo, opp_hi, ring_lo, ring_hi, last_opp_lo, last_opp_hi, last_lo, last_hi,
                 send_sem, recv_sem, local_sem):
    tokens, d_model = x_ref.shape
    half, quarter = tokens // 2, tokens // 4
    d_half = d_model // 2
    in_part = w_in_ref.shape[1]
    out_part = w_out_ref.shape[1]
    chip_rows = CORES * out_part
    real_cols = CORES * in_part
    chip_cols = w_in_all.shape[0]
    me = lax.axis_index("fsdp")
    core = lax.rem(me, CORES)
    chip = me // CORES
    x = lax.rem(chip, ring)
    y = chip // ring

    def wrap(a):
        return lax.rem(a + ring, ring)

    def device(cx, cy):
        return (wrap(cy) * ring + wrap(cx)) * CORES + core

    sends = []
    done = set()

    def send(event, src, dst, target):
        copy = pltpu.make_async_remote_copy(src_ref=src, dst_ref=dst, send_sem=send_sem.at[event],
                                            recv_sem=recv_sem.at[event], device_id={"fsdp": target},
                                            device_id_type=MESH)
        copy.start()
        sends.append(copy)

    def need(event, dst):
        if event in done:
            return
        done.add(event)
        pltpu.make_async_remote_copy(src_ref=dst, dst_ref=dst, send_sem=send_sem.at[event],
                                     recv_sem=recv_sem.at[event], device_id={"fsdp": me},
                                     device_id_type=MESH).wait_recv()

    margin = chip_cols - real_cols
    if margin:
        w_in_all[0:margin] = jnp.zeros((margin, d_model), w_in_all.dtype)
        w_in_all[real_cols:chip_cols] = jnp.zeros((margin, d_model), w_in_all.dtype)

    peer = chip * CORES + (1 - core)
    barrier = pltpu.get_barrier_semaphore()
    pl.semaphore_signal(barrier, inc=1, device_id={"fsdp": peer}, device_id_type=MESH)
    others = [(dx, dy) for dy in range(ring) for dx in range(ring) if dx or dy]
    for dx, dy in others:
        pl.semaphore_signal(barrier, inc=1, device_id={"fsdp": device(x + dx, y + dy)}, device_id_type=MESH)

    phase = lax.rem(real_cols * chip, LANES)

    def in_rows(which):
        return w_in_all.at[pl.ds(pl.multiple_of(phase + which * in_part, 16), in_part)]

    def out_rows(which):
        return w_out_all.at[pl.ds(pl.multiple_of(which * out_part, 16), out_part)]

    local = [
        pltpu.make_async_copy(w_in_ref.at[layer], in_rows(core), local_sem.at[0]),
        pltpu.make_async_copy(w_out_ref.at[layer], out_rows(core), local_sem.at[1]),
    ]
    for copy in local:
        copy.start()

    x_float = x_ref[...].astype(jnp.float32)
    centred = x_float - jnp.mean(x_float, axis=-1, keepdims=True)
    variance = jnp.mean(centred * centred, axis=-1, keepdims=True)
    normed = centred * lax.rsqrt(variance + NORM_EPS) * gain_ref[layer:layer + 1].astype(jnp.float32)
    h_all[y, x] = normed.astype(jnp.bfloat16)

    pl.semaphore_wait(barrier, len(others) + 1)

    def place(part, prim, sec):
        return (x + prim, y + sec) if part == 0 else (x + sec, y + prim)

    def block(part, prim, sec, low, count):
        cx, cy = place(part, prim, sec)
        return h_all.at[wrap(cy), wrap(cx), pl.ds(part * half + low, count)]

    def gather_send(event, part, blk, prim, sec):
        send(event, blk, blk, device(*place(part, prim, sec)))

    steps = (0, -1, 1, 2)

    def base(part):
        return GATHER + 20 * part

    def to_second(part, j):
        e = base(part) + 4 + 4 * j
        blk = block(part, steps[j], 0, 0, half)
        gather_send(e, part, blk, 0, 1)
        gather_send(e + 1, part, blk, 0, -1)

    def got_first(part, which):
        e = base(part)
        if which == -1:
            need(e, block(part, -1, 0, 0, half))
        elif which == 1:
            need(e + 1, block(part, 1, 0, 0, half))
        else:
            need(e + 2, block(part, 2, 0, 0, quarter))
            need(e + 3, block(part, 2, 0, quarter, quarter))

    def got_second(part, j, which):
        e = base(part) + 4 + 4 * j
        dp = steps[j]
        if which == -1:
            need(e, block(part, dp, -1, 0, half))
        elif which == 1:
            need(e + 1, block(part, dp, 1, 0, half))
        else:
            need(e + 2, block(part, dp, 2, 0, quarter))
            need(e + 3, block(part, dp, 2, quarter, quarter))

    def pass_second(part, j):
        e = base(part) + 4 + 4 * j
        dp = steps[j]
        got_second(part, j, -1)
        gather_send(e + 2, part, block(part, dp, -1, 0, quarter), 0, 1)
        got_second(part, j, 1)
        gather_send(e + 3, part, block(part, dp, 1, quarter, quarter), 0, -1)

    for part in (0, 1):
        own = block(part, 0, 0, 0, half)
        gather_send(base(part), part, own, 1, 0)
        gather_send(base(part) + 1, part, own, -1, 0)
    for part in (0, 1):
        to_second(part, 0)
    send(WEIGHT, w_in_ref.at[layer], in_rows(core), peer)
    send(WEIGHT + 1, w_out_ref.at[layer], out_rows(core), peer)
    for part in (0, 1):
        got_first(part, -1)
        gather_send(base(part) + 2, part, block(part, -1, 0, 0, quarter), 1, 0)
        got_first(part, 1)
        gather_send(base(part) + 3, part, block(part, 1, 0, quarter, quarter), -1, 0)
    for part in (0, 1):
        to_second(part, 1)
        to_second(part, 2)
    for part in (0, 1):
        pass_second(part, 0)
    for part in (0, 1):
        got_first(part, 2)
        to_second(part, 3)

    local[0].wait()
    need(WEIGHT, in_rows(1 - core))

    wide = math.gcd(chip_cols, 256)

    def row_product(dy):
        row = wrap(y + dy)
        lhs = h_all[row].reshape(ring * tokens, d_model)

        @pl.loop(0, chip_cols // wide)
        def _(n):
            cols = pl.ds(pl.multiple_of(n * wide, wide), wide)
            res = lax.dot_general(lhs, w_in_all[cols], (((1,), (1,)), ((), ())), preferred_element_type=jnp.float32)
            p_out[row, :, :, cols] = res.astype(jnp.bfloat16).reshape(ring, tokens, wide)

    def row_send(dy):
        row = wrap(y + dy)
        for dx in (2, 1, 3, 0):
            col = wrap(x + dx)
            if dx == 0 and dy == 0:
                p_in[y, x] = p_out[y, x]
            else:
                send(SEND_P + (dy % ring) * ring + dx, p_out.at[row, col], p_in.at[y, x], device(x + dx, y + dy))

    for which in (-1, 1, 2):
        got_second(1, 0, which)
    row_product(0)
    for j in (1, 2):
        for part in (0, 1):
            pass_second(part, j)
    for part in (0, 1):
        pass_second(part, 3)
    row_send(0)
    for dy, j in ((-1, 1), (1, 2), (2, 3)):
        for i in range(ring):
            got_second(0, i, dy)
        for which in (-1, 1, 2):
            got_second(1, j, which)
        row_product(dy)
        row_send(dy)

    for dx, dy in others:
        need(SEND_P + dy * ring + dx, p_in.at[wrap(y - dy), wrap(x - dx)])

    def tile(t):
        pieces = []
        for c in range(ring * ring):
            if c * real_cols < (t + 1) * LANES and (c + 1) * real_cols > t * LANES:
                low = (t - (c * real_cols) // LANES) * LANES
                pieces.append(p_in[c // ring, c % ring, :, low:low + LANES])
        return sum(pieces[1:], pieces[0])

    cos_table = cos_ref[...]
    sin_table = sin_ref[...]

    def rotated(t, scale):
        first = tile(t).astype(jnp.float32)
        second = tile(t + 1).astype(jnp.float32)
        a = first * cos_table - second * sin_table
        b = second * cos_table + first * sin_table
        return jnp.concatenate([(a * scale).astype(jnp.bfloat16), (b * scale).astype(jnp.bfloat16)], axis=-1)

    head_tiles = HEAD_DIM // LANES
    q_tiles = num_heads * head_tiles
    out_tiles = chip_rows // LANES

    def put(t, val):
        c, i = divmod(t, out_tiles)
        mixed_out[c, :, i * LANES:(i + 1) * LANES] = val

    ff_tiles = ring * ring * out_tiles - q_tiles
    for t in range(ff_tiles):
        gate = tile(q_tiles + 4 + t).astype(jnp.float32)
        up = tile(q_tiles + 4 + ff_tiles + t).astype(jnp.float32)
        put(q_tiles + t, (jax.nn.silu(gate) * up).astype(jnp.bfloat16))

    far_first = sorted(others, key=lambda d: -((d[0] == 2) + (d[1] == 2)))
    first_plain = -(-q_tiles // out_tiles)

    def mixed_send(plain):
        for dx, dy in far_first:
            dest = wrap(y + dy) * ring + wrap(x + dx)
            copy = pltpu.make_async_remote_copy(
                src_ref=mixed_out.at[dest], dst_ref=mixed_in.at[y, x], send_sem=send_sem.at[SEND_M + dy * ring + dx],
                recv_sem=recv_sem.at[SEND_M + dy * ring + dx], device_id={"fsdp": device(x + dx, y + dy)},
                device_id_type=MESH)

            @pl.when(dest >= first_plain if plain else dest < first_plain)
            def _():
                copy.start()

            if not plain:
                sends.append(copy)

    mixed_send(True)
    query = jnp.concatenate([rotated(h * head_tiles, HEAD_DIM ** -0.5) for h in range(num_heads)], axis=0)
    key = rotated(q_tiles, 1.0)
    value = jnp.concatenate([tile(q_tiles + 2), tile(q_tiles + 3)], axis=-1)
    k_ref[...] = key
    v_ref[...] = value
    scores = lax.dot_general(query, key, (((1,), (1,)), ((), ())), preferred_element_type=jnp.float32)
    scores = scores.reshape(num_heads, tokens, tokens)
    q_pos = lax.broadcasted_iota(jnp.int32, scores.shape, 1)
    k_pos = lax.broadcasted_iota(jnp.int32, scores.shape, 2)
    scores = jnp.where(q_pos >= k_pos, scores, -1e30)
    weight = jnp.exp(scores - jnp.max(scores, axis=-1, keepdims=True))
    row_sum = jnp.sum(weight, axis=-1, keepdims=True)
    attended = jnp.dot(weight.astype(jnp.bfloat16).reshape(num_heads * tokens, tokens), value,
                       preferred_element_type=jnp.float32).reshape(num_heads, tokens, HEAD_DIM)
    attended = (attended / row_sum).astype(jnp.bfloat16)
    for h in range(num_heads):
        for i in range(head_tiles):
            put(h * head_tiles + i, attended[h, :, i * LANES:(i + 1) * LANES])
    mixed_send(False)
    mixed_in[y, x] = mixed_out[chip]
    local[1].wait()
    need(WEIGHT + 1, out_rows(1 - core))

    parts = (part_y, part_x)
    centre = ((y, x), (x, y))

    def lined(f, prim, sec):
        return (x + sec, y + prim) if f == 0 else (x + prim, y + sec)

    def arrived(f, prim):
        for sec in range(ring):
            dx, dy = (-sec, -prim) if f == 0 else (-prim, -sec)
            dx, dy = dx % ring, dy % ring
            if dx or dy:
                need(SEND_M + dy * ring + dx, mixed_in.at[wrap(y - dy), wrap(x - dx)])

    narrow = min(d_half, 256)

    def product(f, prim):
        arrived(f, prim)
        idx = wrap(centre[f][0] + prim)
        lhs = mixed_in[idx] if f == 0 else mixed_in[:, idx]
        lhs = lhs.reshape(ring * tokens, chip_rows)

        @pl.loop(0, d_half // narrow)
        def _(n):
            src = pl.ds(pl.multiple_of(f * d_half + n * narrow, narrow), narrow)
            cols = pl.ds(pl.multiple_of(n * narrow, narrow), narrow)
            res = jnp.dot(lhs, w_out_all[:, src], preferred_element_type=jnp.float32)
            parts[f][idx, :, :, cols] = res.reshape(ring, tokens, narrow)

    lo, hi = pl.ds(0, ring // 2), pl.ds(ring // 2, ring // 2)
    t_lo, t_hi = pl.ds(0, half), pl.ds(half, half)

    def event(f, i):
        return REDUCE + 12 * f + i

    def at(f, prim):
        return wrap(centre[f][0] + prim)

    def toward(f, prim, sec):
        return device(*lined(f, prim, sec))

    for f in (0, 1):
        product(f, 2)
        send(event(f, 0), parts[f].at[at(f, 2), lo], opp_lo.at[f], toward(f, 1, 0))
        send(event(f, 1), parts[f].at[at(f, 2), hi], opp_hi.at[f], toward(f, -1, 0))
    for f in (0, 1):
        product(f, 1)
        send(event(f, 2), parts[f].at[at(f, 1), hi], ring_lo.at[f, hi], toward(f, 1, 0))
        product(f, -1)
        send(event(f, 3), parts[f].at[at(f, -1), lo], ring_hi.at[f, lo], toward(f, -1, 0))
    for f in (0, 1):
        product(f, 0)
    for f in (0, 1):
        need(event(f, 0), opp_lo.at[f])
        parts[f][at(f, 1), lo] = parts[f][at(f, 1), lo] + opp_lo[f]
        send(event(f, 4), parts[f].at[at(f, 1), lo], ring_lo.at[f, lo], toward(f, 1, 0))
        need(event(f, 1), opp_hi.at[f])
        parts[f][at(f, -1), hi] = parts[f][at(f, -1), hi] + opp_hi[f]
        send(event(f, 5), parts[f].at[at(f, -1), hi], ring_hi.at[f, hi], toward(f, -1, 0))

    def second(f, sec):
        return wrap(centre[f][1] + sec)

    for f in (0, 1):
        need(event(f, 2), ring_lo.at[f, hi])
        need(event(f, 3), ring_hi.at[f, lo])
        need(event(f, 4), ring_lo.at[f, lo])
        need(event(f, 5), ring_hi.at[f, hi])
        mid = at(f, 0)
        parts[f][mid] = parts[f][mid] + ring_lo[f] + ring_hi[f]
        send(event(f, 6), parts[f].at[mid, second(f, 2), t_lo], last_opp_lo.at[f], toward(f, 0, 1))
        send(event(f, 7), parts[f].at[mid, second(f, 2), t_hi], last_opp_hi.at[f], toward(f, 0, -1))
        send(event(f, 8), parts[f].at[mid, second(f, 1), t_hi], last_lo.at[f, t_hi], toward(f, 0, 1))
        send(event(f, 9), parts[f].at[mid, second(f, -1), t_lo], last_hi.at[f, t_lo], toward(f, 0, -1))
    for f in (0, 1):
        mid = at(f, 0)
        need(event(f, 6), last_opp_lo.at[f])
        parts[f][mid, second(f, 1), t_lo] = parts[f][mid, second(f, 1), t_lo] + last_opp_lo[f]
        send(event(f, 10), parts[f].at[mid, second(f, 1), t_lo], last_lo.at[f, t_lo], toward(f, 0, 1))
        need(event(f, 7), last_opp_hi.at[f])
        parts[f][mid, second(f, -1), t_hi] = parts[f][mid, second(f, -1), t_hi] + last_opp_hi[f]
        send(event(f, 11), parts[f].at[mid, second(f, -1), t_hi], last_hi.at[f, t_hi], toward(f, 0, -1))
    for f in (0, 1):
        need(event(f, 8), last_lo.at[f, t_hi])
        need(event(f, 9), last_hi.at[f, t_lo])
        need(event(f, 10), last_lo.at[f, t_lo])
        need(event(f, 11), last_hi.at[f, t_hi])
        out_sum = parts[f][at(f, 0), second(f, 0)] + last_lo[f] + last_hi[f]
        cols = slice(f * d_half, (f + 1) * d_half)
        y_ref[:, cols] = (x_ref[:, cols].astype(jnp.float32) + out_sum).astype(jnp.bfloat16)
    for copy in sends:
        copy.wait_send()


def parallel_layer(hidden, gain, w_in_rows, w_out_part, tables, ring, num_heads, layer):
    batch, tokens, d_model = hidden.shape
    out_part = w_out_part.shape[1]
    real_cols = CORES * w_in_rows.shape[1]
    margin = max((real_cols * c) % LANES for c in range(ring * ring))
    padded_cols = -(-(real_cols + margin) // LANES) * LANES
    chip_rows = CORES * out_part
    d_half = d_model // 2
    bf16, f32 = jnp.bfloat16, jnp.float32
    vmem = pl.BlockSpec(memory_space=pltpu.VMEM)
    anywhere = pl.BlockSpec(memory_space=pl.ANY)
    out, k_rot, value = pl.pallas_call(
        functools.partial(layer_kernel, ring, num_heads, layer),
        out_shape=(
            jax.ShapeDtypeStruct((tokens, d_model), bf16),
            jax.ShapeDtypeStruct((tokens, HEAD_DIM), bf16),
            jax.ShapeDtypeStruct((tokens, HEAD_DIM), bf16),
        ),
        in_specs=[vmem, vmem, anywhere, anywhere, vmem, vmem],
        out_specs=(vmem, vmem, vmem),
        scratch_shapes=[
            pltpu.VMEM((ring, ring, tokens, d_model), bf16),
            pltpu.VMEM((padded_cols, d_model), bf16),
            pltpu.VMEM((chip_rows, d_model), bf16),
            pltpu.VMEM((ring, ring, tokens, padded_cols), bf16),
            pltpu.VMEM((ring, ring, tokens, padded_cols), bf16),
            pltpu.VMEM((ring * ring, tokens, chip_rows), bf16),
            pltpu.VMEM((ring, ring, tokens, chip_rows), bf16),
            pltpu.VMEM((ring, ring, tokens, d_half), f32),
            pltpu.VMEM((ring, ring, tokens, d_half), f32),
            pltpu.VMEM((2, ring // 2, tokens, d_half), f32),
            pltpu.VMEM((2, ring // 2, tokens, d_half), f32),
            pltpu.VMEM((2, ring, tokens, d_half), f32),
            pltpu.VMEM((2, ring, tokens, d_half), f32),
            pltpu.VMEM((2, tokens // 2, d_half), f32),
            pltpu.VMEM((2, tokens // 2, d_half), f32),
            pltpu.VMEM((2, tokens, d_half), f32),
            pltpu.VMEM((2, tokens, d_half), f32),
            pltpu.SemaphoreType.DMA((EVENTS,)),
            pltpu.SemaphoreType.DMA((EVENTS,)),
            pltpu.SemaphoreType.DMA((2,)),
        ],
        compiler_params=pltpu.CompilerParams(collective_id=layer, has_side_effects=True, vmem_limit_bytes=62 * 2 ** 20),
        name="layer",
    )(hidden.reshape(tokens, d_model), gain, w_in_rows, w_out_part, *tables)
    return out.reshape(hidden.shape), k_rot.reshape(batch, tokens, HEAD_DIM), value.reshape(batch, tokens, HEAD_DIM)


def solution(mesh):
    batch_axes = ("dp", "fsdp")
    group = mesh.shape["fsdp"]
    ring = math.isqrt(group // CORES)
    if ring != 4 or ring * ring * CORES != group:
        raise ValueError("unsupported group")

    def device_program(x_local, gain, w_in_local, w_out_local):
        layers, d_model, in_part = w_in_local.shape
        out_rows = w_out_local.shape[1] * group
        ff_dim = in_part * group - out_rows - 2 * HEAD_DIM
        num_heads = (out_rows - ff_dim) // HEAD_DIM
        w_in_rows = jnp.swapaxes(w_in_local, 1, 2)
        hidden = x_local
        tables = rope_tables(x_local.shape[1])
        key_list = []
        value_list = []
        for layer in range(layers):
            hidden, k_rot, value = parallel_layer(hidden, gain, w_in_rows, w_out_local, tables, ring, num_heads, layer)
            key_list.append(k_rot)
            value_list.append(value)
        return hidden, jnp.stack(key_list), jnp.stack(value_list)

    return jax.shard_map(
        device_program,
        mesh=mesh,
        in_specs=(P(batch_axes, None, None), P(None, None), P(None, None, "fsdp"), P(None, "fsdp", None)),
        out_specs=(P(batch_axes, None, None), P(None, batch_axes, None, None), P(None, batch_axes, None, None)),
        check_vma=False,
    )
```

```python
import functools
import math

import jax
import jax.numpy as jnp
from jax import lax
from jax.experimental import pallas as pl
from jax.experimental.pallas import tpu as pltpu
import numpy as np
from jax.sharding import PartitionSpec as P

HEAD_DIM = 256
ROPE_BASE = 10000.0
NORM_EPS = 1e-6
LANES = 128
CORES = 2
MESH = pl.DeviceIdType.MESH


def rope_tables(seq_len):
    half_dim = HEAD_DIM // 2
    inv_freq = np.float32(ROPE_BASE) ** (-np.arange(half_dim, dtype=np.float32) / np.float32(half_dim))
    angle = np.arange(seq_len, dtype=np.float32)[:, None] * inv_freq[None, :].astype(np.float32)
    return jnp.asarray(np.cos(angle), jnp.float32), jnp.asarray(np.sin(angle), jnp.float32)


GATHER, SEND_P, SEND_M, REDUCE, WEIGHT = 0, 40, 56, 72, 96
EVENTS = 98


def layers_kernel(ring, num_heads, x_ref, gain_ref, w_in_ref, w_out_ref, cos_ref, sin_ref, y_ref, k_ref, v_ref,
                 h_all, p_out, p_in, mixed_out, mixed_in, part_y, part_x,
                 opp_lo, opp_hi, ring_lo, ring_hi, last_opp_lo, last_opp_hi, last_lo, last_hi,
                 send_sem, recv_sem, local_sem, *weights):
    tokens, d_model = x_ref.shape
    half, quarter = tokens // 2, tokens // 4
    d_half = d_model // 2
    in_part = w_in_ref.shape[1]
    out_part = w_out_ref.shape[1]
    chip_rows = CORES * out_part
    real_cols = CORES * in_part
    layers = len(weights) // 2
    w_in_all, w_out_all = weights[:layers], weights[layers:]
    chip_cols = w_in_all[0].shape[0]
    me = lax.axis_index("fsdp")
    core = lax.rem(me, CORES)
    chip = me // CORES
    x = lax.rem(chip, ring)
    y = chip // ring

    def wrap(a):
        return lax.rem(a + ring, ring)

    def device(cx, cy):
        return (wrap(cy) * ring + wrap(cx)) * CORES + core

    margin = chip_cols - real_cols
    if margin:
        for buf in w_in_all:
            buf[0:margin] = jnp.zeros((margin, d_model), buf.dtype)
            buf[real_cols:chip_cols] = jnp.zeros((margin, d_model), buf.dtype)

    peer = chip * CORES + (1 - core)
    barrier = pltpu.get_barrier_semaphore()
    pl.semaphore_signal(barrier, inc=1, device_id={"fsdp": peer}, device_id_type=MESH)
    others = [(dx, dy) for dy in range(ring) for dx in range(ring) if dx or dy]
    for dx, dy in others:
        pl.semaphore_signal(barrier, inc=1, device_id={"fsdp": device(x + dx, y + dy)}, device_id_type=MESH)

    phase = lax.rem(real_cols * chip, LANES)

    def in_rows(layer, which):
        return w_in_all[layer].at[pl.ds(pl.multiple_of(phase + which * in_part, 16), in_part)]

    def out_rows(layer, which):
        return w_out_all[layer].at[pl.ds(pl.multiple_of(which * out_part, 16), out_part)]

    local = []
    for layer in range(layers):
        local.append(pltpu.make_async_copy(w_in_ref.at[layer], in_rows(layer, core), local_sem.at[2 * layer]))
        local.append(pltpu.make_async_copy(w_out_ref.at[layer], out_rows(layer, core), local_sem.at[2 * layer + 1]))
    for copy in local:
        copy.start()

    def run_layer(layer):
        first = EVENTS * layer
        source = x_ref if layer == 0 else y_ref
        sends = []
        gathers = []
        done = set()

        def send(event, src, dst, target):
            copy = pltpu.make_async_remote_copy(src_ref=src, dst_ref=dst, send_sem=send_sem.at[first + event],
                                                recv_sem=recv_sem.at[first + event], device_id={"fsdp": target},
                                                device_id_type=MESH)
            copy.start()
            (gathers if event < SEND_P else sends).append(copy)

        def need(event, dst):
            if event in done:
                return
            done.add(event)
            pltpu.make_async_remote_copy(src_ref=dst, dst_ref=dst, send_sem=send_sem.at[first + event],
                                         recv_sem=recv_sem.at[first + event], device_id={"fsdp": me},
                                         device_id_type=MESH).wait_recv()

        def send_weights(which):
            shift = EVENTS * (which - layer)
            send(shift + WEIGHT, w_in_ref.at[which], in_rows(which, core), peer)
            send(shift + WEIGHT + 1, w_out_ref.at[which], out_rows(which, core), peer)

        x_float = source[...].astype(jnp.float32)
        centred = x_float - jnp.mean(x_float, axis=-1, keepdims=True)
        variance = jnp.mean(centred * centred, axis=-1, keepdims=True)
        normed = centred * lax.rsqrt(variance + NORM_EPS) * gain_ref[layer:layer + 1].astype(jnp.float32)
        h_all[y, x] = normed.astype(jnp.bfloat16)

        if layer == 0:
            pl.semaphore_wait(barrier, len(others) + 1)

        def place(part, prim, sec):
            return (x + prim, y + sec) if part == 0 else (x + sec, y + prim)

        def block(part, prim, sec, low, count):
            cx, cy = place(part, prim, sec)
            return h_all.at[wrap(cy), wrap(cx), pl.ds(part * half + low, count)]

        def gather_send(event, part, blk, prim, sec):
            send(event, blk, blk, device(*place(part, prim, sec)))

        steps = (0, -1, 1, 2)

        def base(part):
            return GATHER + 20 * part

        def to_second(part, j):
            e = base(part) + 4 + 4 * j
            blk = block(part, steps[j], 0, 0, half)
            gather_send(e, part, blk, 0, 1)
            gather_send(e + 1, part, blk, 0, -1)

        def got_first(part, which):
            e = base(part)
            if which == -1:
                need(e, block(part, -1, 0, 0, half))
            elif which == 1:
                need(e + 1, block(part, 1, 0, 0, half))
            else:
                need(e + 2, block(part, 2, 0, 0, quarter))
                need(e + 3, block(part, 2, 0, quarter, quarter))

        def got_second(part, j, which):
            e = base(part) + 4 + 4 * j
            dp = steps[j]
            if which == -1:
                need(e, block(part, dp, -1, 0, half))
            elif which == 1:
                need(e + 1, block(part, dp, 1, 0, half))
            else:
                need(e + 2, block(part, dp, 2, 0, quarter))
                need(e + 3, block(part, dp, 2, quarter, quarter))

        def pass_second(part, j):
            e = base(part) + 4 + 4 * j
            dp = steps[j]
            got_second(part, j, -1)
            gather_send(e + 2, part, block(part, dp, -1, 0, quarter), 0, 1)
            got_second(part, j, 1)
            gather_send(e + 3, part, block(part, dp, 1, quarter, quarter), 0, -1)

        for part in (0, 1):
            own = block(part, 0, 0, 0, half)
            gather_send(base(part), part, own, 1, 0)
            gather_send(base(part) + 1, part, own, -1, 0)
        for part in (0, 1):
            to_second(part, 0)
        if layer == 0:
            send_weights(0)
        for part in (0, 1):
            got_first(part, -1)
            gather_send(base(part) + 2, part, block(part, -1, 0, 0, quarter), 1, 0)
            got_first(part, 1)
            gather_send(base(part) + 3, part, block(part, 1, 0, quarter, quarter), -1, 0)
        for part in (0, 1):
            to_second(part, 1)
            to_second(part, 2)
        for part in (0, 1):
            pass_second(part, 0)
        for part in (0, 1):
            got_first(part, 2)
            to_second(part, 3)

        local[2 * layer].wait()
        need(WEIGHT, in_rows(layer, 1 - core))

        wide = math.gcd(chip_cols, 256)

        def row_product(dy):
            row = wrap(y + dy)
            lhs = h_all[row].reshape(ring * tokens, d_model)

            @pl.loop(0, chip_cols // wide)
            def _(n):
                cols = pl.ds(pl.multiple_of(n * wide, wide), wide)
                res = lax.dot_general(lhs, w_in_all[layer][cols], (((1,), (1,)), ((), ())), preferred_element_type=jnp.float32)
                p_out[row, :, :, cols] = res.astype(jnp.bfloat16).reshape(ring, tokens, wide)

        def row_send(dy):
            row = wrap(y + dy)
            for dx in (2, 1, 3, 0):
                col = wrap(x + dx)
                if dx == 0 and dy == 0:
                    p_in[y, x] = p_out[y, x]
                else:
                    send(SEND_P + (dy % ring) * ring + dx, p_out.at[row, col], p_in.at[y, x], device(x + dx, y + dy))

        for which in (-1, 1, 2):
            got_second(1, 0, which)
        row_product(0)
        for j in (1, 2):
            for part in (0, 1):
                pass_second(part, j)
        for part in (0, 1):
            pass_second(part, 3)
        row_send(0)
        for dy, j in ((-1, 1), (1, 2), (2, 3)):
            for i in range(ring):
                got_second(0, i, dy)
            for which in (-1, 1, 2):
                got_second(1, j, which)
            row_product(dy)
            row_send(dy)

        for dx, dy in others:
            need(SEND_P + dy * ring + dx, p_in.at[wrap(y - dy), wrap(x - dx)])
        if layer + 1 < layers:
            send_weights(layer + 1)

        def tile(t):
            pieces = []
            for c in range(ring * ring):
                if c * real_cols < (t + 1) * LANES and (c + 1) * real_cols > t * LANES:
                    low = (t - (c * real_cols) // LANES) * LANES
                    pieces.append(p_in[c // ring, c % ring, :, low:low + LANES])
            return sum(pieces[1:], pieces[0])

        cos_table = cos_ref[...]
        sin_table = sin_ref[...]

        def rotated(t, scale):
            first = tile(t).astype(jnp.float32)
            second = tile(t + 1).astype(jnp.float32)
            a = first * cos_table - second * sin_table
            b = second * cos_table + first * sin_table
            return jnp.concatenate([(a * scale).astype(jnp.bfloat16), (b * scale).astype(jnp.bfloat16)], axis=-1)

        head_tiles = HEAD_DIM // LANES
        q_tiles = num_heads * head_tiles
        out_tiles = chip_rows // LANES

        def put(t, val):
            c, i = divmod(t, out_tiles)
            mixed_out[c, :, i * LANES:(i + 1) * LANES] = val

        ff_tiles = ring * ring * out_tiles - q_tiles
        for t in range(ff_tiles):
            gate = tile(q_tiles + 4 + t).astype(jnp.float32)
            up = tile(q_tiles + 4 + ff_tiles + t).astype(jnp.float32)
            put(q_tiles + t, (jax.nn.silu(gate) * up).astype(jnp.bfloat16))

        far_first = sorted(others, key=lambda d: -((d[0] == 2) + (d[1] == 2)))
        first_plain = -(-q_tiles // out_tiles)

        def mixed_send(plain):
            for dx, dy in far_first:
                dest = wrap(y + dy) * ring + wrap(x + dx)
                copy = pltpu.make_async_remote_copy(
                    src_ref=mixed_out.at[dest], dst_ref=mixed_in.at[y, x], send_sem=send_sem.at[first + SEND_M + dy * ring + dx],
                    recv_sem=recv_sem.at[first + SEND_M + dy * ring + dx], device_id={"fsdp": device(x + dx, y + dy)},
                    device_id_type=MESH)

                @pl.when(dest >= first_plain if plain else dest < first_plain)
                def _():
                    copy.start()

                if not plain:
                    sends.append(copy)

        for copy in gathers:
            copy.wait_send()
        mixed_send(True)
        query = jnp.concatenate([rotated(h * head_tiles, HEAD_DIM ** -0.5) for h in range(num_heads)], axis=0)
        key = rotated(q_tiles, 1.0)
        value = jnp.concatenate([tile(q_tiles + 2), tile(q_tiles + 3)], axis=-1)
        k_ref[layer] = key
        v_ref[layer] = value
        scores = lax.dot_general(query, key, (((1,), (1,)), ((), ())), preferred_element_type=jnp.float32)
        scores = scores.reshape(num_heads, tokens, tokens)
        q_pos = lax.broadcasted_iota(jnp.int32, scores.shape, 1)
        k_pos = lax.broadcasted_iota(jnp.int32, scores.shape, 2)
        scores = jnp.where(q_pos >= k_pos, scores, -1e30)
        weight = jnp.exp(scores - jnp.max(scores, axis=-1, keepdims=True))
        row_sum = jnp.sum(weight, axis=-1, keepdims=True)
        attended = jnp.dot(weight.astype(jnp.bfloat16).reshape(num_heads * tokens, tokens), value,
                           preferred_element_type=jnp.float32).reshape(num_heads, tokens, HEAD_DIM)
        attended = (attended / row_sum).astype(jnp.bfloat16)
        for h in range(num_heads):
            for i in range(head_tiles):
                put(h * head_tiles + i, attended[h, :, i * LANES:(i + 1) * LANES])
        mixed_send(False)
        mixed_in[y, x] = mixed_out[chip]
        local[2 * layer + 1].wait()
        need(WEIGHT + 1, out_rows(layer, 1 - core))

        parts = (part_y, part_x)
        centre = ((y, x), (x, y))

        def lined(f, prim, sec):
            return (x + sec, y + prim) if f == 0 else (x + prim, y + sec)

        def arrived(f, prim):
            for sec in range(ring):
                dx, dy = (-sec, -prim) if f == 0 else (-prim, -sec)
                dx, dy = dx % ring, dy % ring
                if dx or dy:
                    need(SEND_M + dy * ring + dx, mixed_in.at[wrap(y - dy), wrap(x - dx)])

        narrow = min(d_half, 256)

        def product(f, prim):
            arrived(f, prim)
            idx = wrap(centre[f][0] + prim)
            lhs = mixed_in[idx] if f == 0 else mixed_in[:, idx]
            lhs = lhs.reshape(ring * tokens, chip_rows)

            @pl.loop(0, d_half // narrow)
            def _(n):
                src = pl.ds(pl.multiple_of(f * d_half + n * narrow, narrow), narrow)
                cols = pl.ds(pl.multiple_of(n * narrow, narrow), narrow)
                res = jnp.dot(lhs, w_out_all[layer][:, src], preferred_element_type=jnp.float32)
                parts[f][idx, :, :, cols] = res.reshape(ring, tokens, narrow)

        lo, hi = pl.ds(0, ring // 2), pl.ds(ring // 2, ring // 2)
        t_lo, t_hi = pl.ds(0, half), pl.ds(half, half)

        def event(f, i):
            return REDUCE + 12 * f + i

        def at(f, prim):
            return wrap(centre[f][0] + prim)

        def toward(f, prim, sec):
            return device(*lined(f, prim, sec))

        for f in (0, 1):
            product(f, 2)
            send(event(f, 0), parts[f].at[at(f, 2), lo], opp_lo.at[f], toward(f, 1, 0))
            send(event(f, 1), parts[f].at[at(f, 2), hi], opp_hi.at[f], toward(f, -1, 0))
        for f in (0, 1):
            product(f, 1)
            send(event(f, 2), parts[f].at[at(f, 1), hi], ring_lo.at[f, hi], toward(f, 1, 0))
            product(f, -1)
            send(event(f, 3), parts[f].at[at(f, -1), lo], ring_hi.at[f, lo], toward(f, -1, 0))
        for f in (0, 1):
            product(f, 0)
        for f in (0, 1):
            need(event(f, 0), opp_lo.at[f])
            parts[f][at(f, 1), lo] = parts[f][at(f, 1), lo] + opp_lo[f]
            send(event(f, 4), parts[f].at[at(f, 1), lo], ring_lo.at[f, lo], toward(f, 1, 0))
            need(event(f, 1), opp_hi.at[f])
            parts[f][at(f, -1), hi] = parts[f][at(f, -1), hi] + opp_hi[f]
            send(event(f, 5), parts[f].at[at(f, -1), hi], ring_hi.at[f, hi], toward(f, -1, 0))

        def second(f, sec):
            return wrap(centre[f][1] + sec)

        for f in (0, 1):
            need(event(f, 2), ring_lo.at[f, hi])
            need(event(f, 3), ring_hi.at[f, lo])
            need(event(f, 4), ring_lo.at[f, lo])
            need(event(f, 5), ring_hi.at[f, hi])
            mid = at(f, 0)
            parts[f][mid] = parts[f][mid] + ring_lo[f] + ring_hi[f]
            send(event(f, 6), parts[f].at[mid, second(f, 2), t_lo], last_opp_lo.at[f], toward(f, 0, 1))
            send(event(f, 7), parts[f].at[mid, second(f, 2), t_hi], last_opp_hi.at[f], toward(f, 0, -1))
            send(event(f, 8), parts[f].at[mid, second(f, 1), t_hi], last_lo.at[f, t_hi], toward(f, 0, 1))
            send(event(f, 9), parts[f].at[mid, second(f, -1), t_lo], last_hi.at[f, t_lo], toward(f, 0, -1))
        for f in (0, 1):
            mid = at(f, 0)
            need(event(f, 6), last_opp_lo.at[f])
            parts[f][mid, second(f, 1), t_lo] = parts[f][mid, second(f, 1), t_lo] + last_opp_lo[f]
            send(event(f, 10), parts[f].at[mid, second(f, 1), t_lo], last_lo.at[f, t_lo], toward(f, 0, 1))
            need(event(f, 7), last_opp_hi.at[f])
            parts[f][mid, second(f, -1), t_hi] = parts[f][mid, second(f, -1), t_hi] + last_opp_hi[f]
            send(event(f, 11), parts[f].at[mid, second(f, -1), t_hi], last_hi.at[f, t_hi], toward(f, 0, -1))
        for f in (0, 1):
            need(event(f, 8), last_lo.at[f, t_hi])
            need(event(f, 9), last_hi.at[f, t_lo])
            need(event(f, 10), last_lo.at[f, t_lo])
            need(event(f, 11), last_hi.at[f, t_hi])
            out_sum = parts[f][at(f, 0), second(f, 0)] + last_lo[f] + last_hi[f]
            cols = slice(f * d_half, (f + 1) * d_half)
            y_ref[:, cols] = (source[:, cols].astype(jnp.float32) + out_sum).astype(jnp.bfloat16)
        for copy in sends:
            copy.wait_send()

    for layer in range(layers):
        run_layer(layer)


def parallel_layers(hidden, gain, w_in_rows, w_out_part, tables, ring, num_heads):
    batch, tokens, d_model = hidden.shape
    layers, out_part, _ = w_out_part.shape
    real_cols = CORES * w_in_rows.shape[1]
    margin = max((real_cols * c) % LANES for c in range(ring * ring))
    padded_cols = -(-(real_cols + margin) // LANES) * LANES
    chip_rows = CORES * out_part
    d_half = d_model // 2
    bf16, f32 = jnp.bfloat16, jnp.float32
    vmem = pl.BlockSpec(memory_space=pltpu.VMEM)
    anywhere = pl.BlockSpec(memory_space=pl.ANY)
    out, k_rot, value = pl.pallas_call(
        functools.partial(layers_kernel, ring, num_heads),
        out_shape=(
            jax.ShapeDtypeStruct((tokens, d_model), bf16),
            jax.ShapeDtypeStruct((layers, tokens, HEAD_DIM), bf16),
            jax.ShapeDtypeStruct((layers, tokens, HEAD_DIM), bf16),
        ),
        in_specs=[vmem, vmem, anywhere, anywhere, vmem, vmem],
        out_specs=(vmem, vmem, vmem),
        scratch_shapes=[
            pltpu.VMEM((ring, ring, tokens, d_model), bf16),
            pltpu.VMEM((ring, ring, tokens, padded_cols), bf16),
            pltpu.VMEM((ring, ring, tokens, padded_cols), bf16),
            pltpu.VMEM((ring * ring, tokens, chip_rows), bf16),
            pltpu.VMEM((ring, ring, tokens, chip_rows), bf16),
            pltpu.VMEM((ring, ring, tokens, d_half), f32),
            pltpu.VMEM((ring, ring, tokens, d_half), f32),
            pltpu.VMEM((2, ring // 2, tokens, d_half), f32),
            pltpu.VMEM((2, ring // 2, tokens, d_half), f32),
            pltpu.VMEM((2, ring, tokens, d_half), f32),
            pltpu.VMEM((2, ring, tokens, d_half), f32),
            pltpu.VMEM((2, tokens // 2, d_half), f32),
            pltpu.VMEM((2, tokens // 2, d_half), f32),
            pltpu.VMEM((2, tokens, d_half), f32),
            pltpu.VMEM((2, tokens, d_half), f32),
            pltpu.SemaphoreType.DMA((layers * EVENTS,)),
            pltpu.SemaphoreType.DMA((layers * EVENTS,)),
            pltpu.SemaphoreType.DMA((2 * layers,)),
        ] + [pltpu.VMEM((padded_cols, d_model), bf16)] * layers + [pltpu.VMEM((chip_rows, d_model), bf16)] * layers,
        compiler_params=pltpu.CompilerParams(collective_id=0, has_side_effects=True, vmem_limit_bytes=62 * 2 ** 20),
        name="layers",
    )(hidden.reshape(tokens, d_model), gain, w_in_rows, w_out_part, *tables)
    caches = (layers, batch, tokens, HEAD_DIM)
    return out.reshape(hidden.shape), k_rot.reshape(caches), value.reshape(caches)


def solution(mesh):
    batch_axes = ("dp", "fsdp")
    group = mesh.shape["fsdp"]
    ring = math.isqrt(group // CORES)
    if ring != 4 or ring * ring * CORES != group:
        raise ValueError("unsupported group")

    def device_program(x_local, gain, w_in_local, w_out_local):
        layers, d_model, in_part = w_in_local.shape
        out_rows = w_out_local.shape[1] * group
        ff_dim = in_part * group - out_rows - 2 * HEAD_DIM
        num_heads = (out_rows - ff_dim) // HEAD_DIM
        w_in_rows = jnp.swapaxes(w_in_local, 1, 2)
        tables = rope_tables(x_local.shape[1])
        return parallel_layers(x_local, gain, w_in_rows, w_out_local, tables, ring, num_heads)

    return jax.shard_map(
        device_program,
        mesh=mesh,
        in_specs=(P(batch_axes, None, None), P(None, None), P(None, None, "fsdp"), P(None, "fsdp", None)),
        out_specs=(P(batch_axes, None, None), P(None, batch_axes, None, None), P(None, batch_axes, None, None)),
        check_vma=False,
    )
```
